32 devices in a mesh: dom: 16 (over z, y, x), mp: 2 (over core).
Axes of the slice: x: 2, y: 2, z: 4, core: 2. Of those that a mesh axis runs over, the one named last changes fastest.
Arguments:
- table: bfloat16 [65536, 768], P('dom', 'mp'), may hold values from -6 to 6
- weight_a: bfloat16 [1536, 512], P(None, 'mp'), may hold values from -0.15625 to 0.15625
- bias_a: float32 [512], replicated, may hold values from -3 to 3
- weight_b: bfloat16 [1024, 512], P(None, 'mp'), may hold values from -0.25 to 0.25
- bias_b: float32 [512], replicated, may hold values from -3 to 3
- requests: int32 [16, 16, 128], P('dom'), may hold values from 0 to 4095
- near_a: int32 [16384, 10], P('dom'), may hold values from 0 to 2047
- self_a: int32 [16384], P('dom'), may hold values from 0 to 2047
- count_a: int32 [16384], P('dom'), may hold values from 1 to 10
- near_b: int32 [4096, 5], P('dom'), may hold values from 0 to 1023
- self_b: int32 [4096], P('dom'), may hold values from 0 to 1023
- count_b: int32 [4096], P('dom'), may hold values from 1 to 5
Outputs:
- embedding: bfloat16 [4096, 512], P('dom', 'mp')
The draws below stay inside these ranges and needn't reach their ends.
Inputs may be any that keep to these rules, and one draw needn't show every extreme that they name: `requests`: local row indices at the owner. `near_a`: slots of the same minibatch; entries at j >= count_a are padding. `near_b`: positions within the same minibatch; entries at j >= count_b are padding.
All inputs are finite; a program needn't handle non-finite values.
Results may differ from the reference program's by a relative error of at most 0.0074.
Values may be sent and summed in bfloat16 or wider, within the bound.
A program may use at most 64 MiB of HBM per device.

```python
import jax
import jax.numpy as jnp
from jax import lax

F = 768
H = 512
FAN_A = 10
FAN_B = 5
SEEDS_DEV = 256
NODE_DEV = 4096
HOP_DEV = 1024
SLOTS_DEV = 2048
NODES = 65536
HOPS = 16384
SEEDS = 4096
N_DOM = 16


def set_ends(values, stream_key, smallest, high):
    index_at = [jax.random.randint(jax.random.fold_in(stream_key, axis), (), 0, length) for axis, length in enumerate(values.shape)]
    widest = values.shape.index(max(values.shape))
    beside = index_at[:widest] + [(index_at[widest] + 1) % values.shape[widest]] + index_at[widest + 1:]
    return values.at[tuple(index_at)].set(smallest).at[tuple(beside)].set(high)


def level_of(rng, dims, split, smallest, high):
    def one(axis_at, blocks):
        heights = jax.random.uniform(jax.random.fold_in(jax.random.fold_in(rng, 6), axis_at), (blocks,), jnp.float32, smallest / len(split), high / len(split))
        return jnp.repeat(jnp.exp(heights), dims[axis_at] // blocks).reshape((-1,) + (1,) * (len(dims) - axis_at - 1))

    level = one(*split[0])
    for cut in split[1:]:
        level = level * one(*cut)
    return level


def centred(rng, dims, width, most, shards=(), kind=jnp.bfloat16):
    loudness = level_of(rng, dims, shards, -0.22, 0.18) if shards else 1.0
    values = jax.random.normal(rng, dims, jnp.float32) * width * loudness
    return jnp.minimum(jnp.maximum(values, -most), most).astype(kind)


def setup_inputs(seed: int = 0) -> dict:
    splits = jax.random.split(jax.random.key(seed), 13)
    table = centred(splits[0], (NODES, F), 1.0, 6.0, ((0, 16), (1, 2)))
    weight_a = centred(splits[1], (2 * F, H), (2 * F) ** -0.5, 0.15625, ((1, 2),))
    bias_a = centred(splits[2], (H,), 0.5, 3.0, (), jnp.float32)
    weight_b = centred(splits[3], (2 * H, H), H ** -0.5, 0.25, ((1, 2),))
    bias_b = centred(splits[4], (H,), 0.5, 3.0, (), jnp.float32)
    requests = set_ends(jax.random.randint(splits[5], (N_DOM, N_DOM, SLOTS_DEV // N_DOM), 0, NODE_DEV), jax.random.fold_in(splits[5], 1), 0, NODE_DEV - 1).astype(jnp.int32)
    near_a = set_ends(jax.random.randint(splits[6], (HOPS, FAN_A), 0, SLOTS_DEV), jax.random.fold_in(splits[6], 1), 0, SLOTS_DEV - 1).astype(jnp.int32)
    self_a = set_ends(jax.random.randint(splits[7], (HOPS,), 0, SLOTS_DEV), jax.random.fold_in(splits[7], 1), 0, SLOTS_DEV - 1).astype(jnp.int32)
    count_a = set_ends(jax.random.randint(splits[8], (HOPS,), 1, FAN_A + 1), jax.random.fold_in(splits[8], 1), 1, FAN_A).astype(jnp.int32)
    near_b = set_ends(jax.random.randint(splits[9], (SEEDS, FAN_B), 0, HOP_DEV), jax.random.fold_in(splits[9], 1), 0, HOP_DEV - 1).astype(jnp.int32)
    self_b = set_ends(jax.random.randint(splits[10], (SEEDS,), 0, HOP_DEV), jax.random.fold_in(splits[10], 1), 0, HOP_DEV - 1).astype(jnp.int32)
    count_b = set_ends(jax.random.randint(splits[11], (SEEDS,), 1, FAN_B + 1), jax.random.fold_in(splits[11], 1), 1, FAN_B).astype(jnp.int32)
    return {"table": table, "weight_a": weight_a, "bias_a": bias_a, "weight_b": weight_b, "bias_b": bias_b, "requests": requests, "near_a": near_a, "self_a": self_a, "count_a": count_a, "near_b": near_b, "self_b": self_b, "count_b": count_b}


def mean_rows(source, neighbours, counts):
    running = jnp.zeros((neighbours.shape[0], source.shape[1]), jnp.float32)
    for column in range(neighbours.shape[1]):
        keep_mask = (counts > column)[:, None]
        running = running + jnp.where(keep_mask, source[neighbours[:, column]].astype(jnp.float32), 0.0)
    return (running / counts[:, None].astype(jnp.float32)).astype(jnp.bfloat16)

def reference(table, weight_a, bias_a, weight_b, bias_b, requests, near_a, self_a, count_a, near_b, self_b, count_b):
    offsets = (jnp.arange(N_DOM) * NODE_DEV).astype(jnp.int32)[:, None]

    def per_device(blocks):
        asked, hop_near, hop_self, hop_count, seed_near, seed_self, seed_count = blocks
        row_ids = (asked + offsets).reshape(-1).astype(jnp.int32)
        fetched = table[row_ids]
        mean_a = mean_rows(fetched, hop_near, hop_count)
        inputs_a = jnp.concatenate([fetched[hop_self], mean_a], axis=1)
        before = jnp.dot(inputs_a, weight_a, preferred_element_type=jnp.float32) + bias_a
        hidden_a = jax.nn.relu(before).astype(jnp.bfloat16)
        mean_b = mean_rows(hidden_a, seed_near, seed_count)
        inputs_b = jnp.concatenate([hidden_a[seed_self], mean_b], axis=1)
        state = jax.nn.relu(jnp.dot(inputs_b, weight_b, preferred_element_type=jnp.float32) + bias_b)
        squares = lax.optimization_barrier(jnp.sum(state * state, axis=1, keepdims=True))
        return (state * jnp.sqrt(jnp.float32(H)) / jnp.sqrt(squares + H)).astype(jnp.bfloat16)
    blocks = (requests, near_a.reshape(N_DOM, HOP_DEV, FAN_A), self_a.reshape(N_DOM, HOP_DEV), count_a.reshape(N_DOM, HOP_DEV), near_b.reshape(N_DOM, SEEDS_DEV, FAN_B), self_b.reshape(N_DOM, SEEDS_DEV), count_b.reshape(N_DOM, SEEDS_DEV))
    result = lax.map(per_device, blocks)
    return result.reshape(N_DOM * SEEDS_DEV, H)
```

```python
import functools

import jax
import jax.numpy as jnp
from jax import lax
from jax.experimental import pallas as pl
from jax.experimental.pallas import tpu as pltpu
from jax.sharding import PartitionSpec as P

MESH = pl.DeviceIdType.MESH
VMEM = pl.BlockSpec(memory_space=pltpu.VMEM)
ANY = pl.BlockSpec(memory_space=pl.ANY)
LANE = 128
TILE = 256
DEPTH = 256


def bit(value, k):
    return lax.rem(lax.div(value, 2**k), 2)


def flips(me, n):
    return [2**k * (1 - 2 * bit(me, k)) for k in range((n - 1).bit_length())]


def exchanged(me, flip, mask):
    for k, delta in enumerate(flip):
        me = me + bit(mask, k) * delta
    return me


def mask_of(step, n):
    half = lax.div(step, 2)
    odd = lax.rem(step, 2)
    return (1 - odd) * (n // 2 + half) + odd * (half + 1)


def dot(a, b):
    return jnp.dot(a, b, preferred_element_type=jnp.float32)


def across(pieces):
    return jnp.concatenate(pieces, axis=1)


def index_rows(index, near_ref, own_ref, count_ref):
    fan, rows = near_ref.shape
    count = count_ref[...]
    pieces = [jnp.where(count > j, near_ref[j : j + 1, :], -1) for j in range(fan)]
    pieces += [own_ref[...], count, jnp.zeros((index.shape[1] - fan - 2, rows), jnp.int32)]
    index[...] = jnp.concatenate(pieces, axis=0).T


def build_picks(index_ref, fan, sum_pick, own_pick, inverse, scaled, first, last):
    chunks = sum_pick.shape[0]
    high = 16

    def one(at, carry):
        r0 = pl.multiple_of(at * high, high)
        index = index_ref[pl.ds(r0, high), :]
        lanes = [
            jnp.broadcast_to(index[:, j : j + 1], (high, LANE)).astype(jnp.int16)
            for j in range(fan + 1)
        ]
        count = jnp.broadcast_to(index[:, fan + 1 : fan + 2], (high, LANE)).astype(jnp.float32)
        inverse[pl.ds(r0, high), :] = 1.0 / count
        lane = lax.broadcasted_iota(jnp.int32, (high, LANE), 1)
        one_value, no_value = jnp.bfloat16(1.0), jnp.bfloat16(0.0)
        own_value = count.astype(jnp.bfloat16) if scaled else one_value
        for c in range(chunks):
            column = (lane + c * LANE).astype(jnp.int16)
            total = jnp.where(lanes[0] == column, one_value, no_value)
            for j in range(1, fan):
                total = total + jnp.where(lanes[j] == column, one_value, no_value)
            sum_pick[c, pl.ds(r0, high), :] = total
            own_pick[c, pl.ds(r0, high), :] = jnp.where(lanes[fan] == column, own_value, no_value)
        return carry

    lax.fori_loop(first, last, one, 0)


def main_kernel(
    n,
    asked_any, table_any, near_a_any, self_a_any, count_a_any, near_b_any, self_b_any, count_b_any,
    weight_a_any, bias_a_any, weight_b_any, bias_b_any,
    out_ref,
    asked, table, near_a, self_a, count_a, near_b, self_b, count_b, wa, bias_a, wb, bias_b,
    wide, wanted, wanted_scalar, stage, found, index_a, index_b,
    fetched, sum_a, own_a, sum_b, own_b, inv_a, inv_b, mixed, total, hidden,
    ask_send, ask_recv, send_sem, recv_sem, relay_send, relay_recv, mp_send, mp_recv, load_sem, scalar_sem,
):
    me = lax.axis_index("dom")
    core = lax.axis_index("mp")
    partner = 1 - core
    flip = flips(me, n)
    cols, each = found.shape[1], found.shape[2]
    rows, seeds, slots = inv_a.shape[0], inv_b.shape[0], n * each
    feature, hidden_width = wa.shape[1] // 2, wb.shape[1] // 2
    fan_a, fan_b = near_a.shape[0], near_b.shape[0]
    blocks = wa.shape[0] // 2
    per = max(1, DEPTH // each)
    groups = n // per
    depth = per * each
    deep = depth // LANE

    def peer(step):
        return exchanged(me, flip, mask_of(step, n))

    loads = [
        pltpu.make_async_copy(source, target, load_sem.at[i])
        for i, (source, target) in enumerate(
            [(asked_any, asked), (near_a_any, near_a), (self_a_any, self_a), (count_a_any, count_a),
             (near_b_any, near_b), (self_b_any, self_b), (count_b_any, count_b), (table_any, table),
             (bias_a_any, bias_a), (bias_b_any, bias_b)]
            + [(weight_a_any.at[:, pl.ds(i * LANE, LANE)], wa.at[core * blocks + i]) for i in range(blocks)]
            + [(weight_b_any.at[:, pl.ds(i * LANE, LANE)], wb.at[core * blocks + i]) for i in range(blocks)]
        )
    ]
    for load in loads:
        load.start()

    barrier = pltpu.get_barrier_semaphore()

    def greet(step, carry):
        pl.semaphore_signal(barrier, inc=1, device_id={"dom": peer(step)}, device_id_type=MESH)
        return carry

    lax.fori_loop(0, n - 1, greet, 0)
    pl.semaphore_signal(barrier, inc=1, device_id={"mp": partner}, device_id_type=MESH)

    for load in loads[1:7]:
        load.wait()
    index_rows(index_a, near_a, self_a, count_a)
    index_rows(index_b, near_b, self_b, count_b)
    steps = rows // 16
    build_picks(index_a, fan_a, sum_a, own_a, inv_a, True, 0, steps // 2)

    loads[0].wait()
    wanted[me] = asked[me]
    pl.semaphore_wait(barrier, n)

    def ask(other):
        return pltpu.make_async_remote_copy(
            src_ref=asked.at[other], dst_ref=wanted.at[me],
            send_sem=ask_send.at[other], recv_sem=ask_recv.at[me],
            device_id={"dom": other}, device_id_type=MESH,
        )

    def give(other):
        return pltpu.make_async_remote_copy(
            src_ref=found.at[other], dst_ref=fetched.at[core, me],
            send_sem=send_sem.at[other], recv_sem=recv_sem.at[me],
            device_id={"dom": other}, device_id_type=MESH,
        )

    def over(source, target, send, recv):
        return pltpu.make_async_remote_copy(
            src_ref=source, dst_ref=target, send_sem=send, recv_sem=recv,
            device_id={"mp": partner}, device_id_type=MESH,
        )

    def relay(other):
        return over(fetched.at[core, other], fetched.at[core, other], relay_send.at[other], relay_recv.at[other])

    def send_ask(step, carry):
        ask(peer(step)).start()
        return carry

    lax.fori_loop(0, n - 1, send_ask, 0)
    for load in loads[7:]:
        load.wait()
    shared = [
        over(w.at[core * blocks + i], w.at[core * blocks + i], mp_send.at[s * blocks + i], mp_recv.at[s * blocks + i])
        for s, w in enumerate((wa, wb)) for i in range(blocks)
    ]
    for copy in shared:
        copy.start()

    def widen(tile, carry):
        at = pl.ds(pl.multiple_of(tile * 128, 128), 128)
        for c in range(cols):
            wide[c, at, :] = table[at, c * LANE : (c + 1) * LANE].astype(jnp.float32)
        return carry

    lax.fori_loop(0, table.shape[0] // 128, widen, 0)
    build_picks(index_a, fan_a, sum_a, own_a, inv_a, True, steps // 2, steps)

    def to_scalar(other):
        return pltpu.make_async_copy(wanted.at[other], wanted_scalar.at[other], scalar_sem.at[other])

    def find(other):
        to_scalar(other).wait()
        for k in range(each):
            row = wanted_scalar[other, 0, k]
            for c in range(cols):
                stage[c, k : k + 1, :] = wide[c, pl.ds(row, 1), :]
        for c in range(cols):
            found[other, c] = stage[c].astype(jnp.bfloat16)

    behind = min(3, n)

    def step_peer(step):
        return exchanged(me, flip, jnp.where(step < n - 1, mask_of(step, n), 0))

    def find_and_send(step, carry):
        @pl.when(step < n)
        def _():
            other = step_peer(step)

            @pl.when(step < n - 1)
            def _():
                pltpu.make_async_copy(asked.at[other], wanted.at[other], ask_recv.at[other]).wait()

            to_scalar(other).start()

        @pl.when(step >= behind)
        def _():
            other = step_peer(step - behind)
            find(other)

            @pl.when(step - behind < n - 1)
            def _():
                give(other).start()

        return carry

    lax.fori_loop(0, n + behind, find_and_send, 0)
    fetched[core, me] = found[me]
    build_picks(index_b, fan_b, sum_b, own_b, inv_b, False, 0, seeds // 16)
    total[...] = jnp.zeros_like(total)
    relay(me).start()
    for copy in shared:
        copy.wait()

    group_flip = flips(lax.div(me, per), groups)
    half_groups = max(1, groups // 2)

    def group_of(k):
        j = lax.rem(k, 2) * half_groups + lax.div(k, 2)
        return exchanged(lax.div(me, per), group_flip, j)

    def take(group):
        def arrive(i, carry):
            other = group * per + i

            @pl.when(other != me)
            def _():
                pltpu.make_async_copy(found.at[other], fetched.at[core, other], recv_sem.at[other]).wait()
                relay(other).start()

            return carry

        lax.fori_loop(0, per, arrive, 0)

    def use(group):
        def arrive(i, carry):
            other = group * per + i
            pltpu.make_async_copy(found.at[other], fetched.at[partner, other], relay_recv.at[other]).wait()
            return carry

        lax.fori_loop(0, per, arrive, 0)
        lines = across([
            fetched[h, pl.ds(group * per, per), c].reshape(depth, LANE) for h in range(2) for c in range(cols)
        ])
        for which in range(2):
            at = pl.ds(which * feature, feature)
            for b in range(0, 2 * blocks, 2):
                value = dot(lines, across([wa[b, at, :], wa[b + 1, at, :]])).astype(jnp.bfloat16)
                for i in range(2):
                    mixed[b + i, which * depth : (which + 1) * depth, :] = value[:, i * LANE : (i + 1) * LANE]

        def one_tile(tile, carry):
            at = pl.ds(pl.multiple_of(tile * TILE, TILE), TILE)
            picks = across([p[group * deep + i, at, :] for p in (own_a, sum_a) for i in range(deep)])
            for b in range(blocks):
                total[b, at, :] += dot(picks, across([mixed[2 * b], mixed[2 * b + 1]]))
            return carry

        lax.fori_loop(0, rows // TILE, one_tile, 0)

    def one_group(k, carry):
        @pl.when(k < groups)
        def _():
            take(group_of(k))

        @pl.when(k > 0)
        def _():
            use(group_of(k - 1))

        return carry

    lax.fori_loop(0, groups + 1, one_group, 0)

    def hide(tile, carry):
        at = pl.ds(pl.multiple_of(tile * TILE, TILE), TILE)
        inverse = inv_a[at, :]
        for b in range(blocks):
            for i in range(2):
                cut = slice((2 * b + i) * LANE, (2 * b + i + 1) * LANE)
                value = total[b, at, i * LANE : (i + 1) * LANE] * inverse + bias_a[:, cut]
                hidden[2 * b + i, at, :] = jnp.maximum(value, 0.0).astype(jnp.bfloat16)
        return carry

    lax.fori_loop(0, rows // TILE, hide, 0)

    hidden_all = across([hidden[b] for b in range(2 * blocks)])
    chunks_b = own_b.shape[0]
    own = dot(across([own_b[c] for c in range(chunks_b)]), hidden_all).astype(jnp.bfloat16)
    mean = dot(across([sum_b[c] for c in range(chunks_b)]), hidden_all)
    mean = (mean * across([inv_b[...]] * (2 * blocks))).astype(jnp.bfloat16)
    state = dot(own, across([wb[b, :hidden_width] for b in range(2 * blocks)]))
    state = state + dot(mean, across([wb[b, hidden_width:] for b in range(2 * blocks)]))
    state = jnp.maximum(state + bias_b[...], 0.0)
    squares = jnp.sum(state * state, axis=1, keepdims=True)
    scale = jnp.sqrt(jnp.float32(hidden_width)) / jnp.sqrt(squares + hidden_width)
    state = (state * scale).astype(out_ref.dtype)
    half = out_ref.shape[1]
    for c in range(2):
        @pl.when(core == c)
        def _():
            out_ref[...] = state[:, c * half : (c + 1) * half]

    def finish(step, carry):
        other = peer(step)
        ask(other).wait_send()
        give(other).wait_send()
        relay(other).wait_send()
        return carry

    lax.fori_loop(0, n - 1, finish, 0)
    relay(me).wait_send()


def shards(
    n,
    table,
    weight_a,
    bias_a,
    weight_b,
    bias_b,
    requests,
    near_a,
    self_a,
    count_a,
    near_b,
    self_b,
    count_b,
):
    each = requests.shape[2]
    half, half_hidden = table.shape[1], weight_a.shape[1]
    rows, seeds, slots = near_a.shape[0], near_b.shape[0], n * each
    wide = -(-(near_a.shape[1] + 2) // 8) * 8
    bf16, f32 = jnp.bfloat16, jnp.float32
    cols, blocks = half // LANE, half_hidden // LANE
    depth = max(1, DEPTH // each) * each
    args = (
        requests[0][:, None, :], table,
        near_a.T, self_a[None, :], count_a[None, :], near_b.T, self_b[None, :], count_b[None, :],
        weight_a, bias_a[None, :], weight_b, bias_b[None, :],
    )
    return pl.pallas_call(
        functools.partial(main_kernel, n),
        out_shape=jax.ShapeDtypeStruct((seeds, half_hidden), bf16),
        in_specs=[ANY] * len(args),
        out_specs=VMEM,
        scratch_shapes=[pltpu.VMEM(a.shape, a.dtype) for a in args[:8]] + [
            pltpu.VMEM((2 * blocks, weight_a.shape[0], LANE), bf16),
            pltpu.VMEM(args[9].shape, f32),
            pltpu.VMEM((2 * blocks, weight_b.shape[0], LANE), bf16),
            pltpu.VMEM(args[11].shape, f32),
            pltpu.VMEM((cols, table.shape[0], LANE), f32),
            pltpu.VMEM((n, 1, each), jnp.int32),
            pltpu.SMEM((n, 1, each), jnp.int32),
            pltpu.VMEM((cols, each, LANE), f32),
            pltpu.VMEM((n, cols, each, LANE), bf16),
            pltpu.VMEM((rows, wide), jnp.int32),
            pltpu.VMEM((seeds, wide), jnp.int32),
            pltpu.VMEM((2, n, cols, each, LANE), bf16),
            pltpu.VMEM((slots // LANE, rows, LANE), bf16),
            pltpu.VMEM((slots // LANE, rows, LANE), bf16),
            pltpu.VMEM((rows // LANE, seeds, LANE), bf16),
            pltpu.VMEM((rows // LANE, seeds, LANE), bf16),
            pltpu.VMEM((rows, LANE), f32),
            pltpu.VMEM((seeds, LANE), f32),
            pltpu.VMEM((2 * blocks, 2 * depth, LANE), bf16),
            pltpu.VMEM((blocks, rows, 2 * LANE), f32),
            pltpu.VMEM((2 * blocks, rows, LANE), bf16),
            pltpu.SemaphoreType.DMA((n,)),
            pltpu.SemaphoreType.DMA((n,)),
            pltpu.SemaphoreType.DMA((n,)),
            pltpu.SemaphoreType.DMA((n,)),
            pltpu.SemaphoreType.DMA((n,)),
            pltpu.SemaphoreType.DMA((n,)),
            pltpu.SemaphoreType.DMA((2 * blocks,)),
            pltpu.SemaphoreType.DMA((2 * blocks,)),
            pltpu.SemaphoreType.DMA((10 + 2 * blocks,)),
            pltpu.SemaphoreType.DMA((n,)),
        ],
        compiler_params=pltpu.CompilerParams(
            collective_id=0, has_side_effects=True, vmem_limit_bytes=60 * 1024 * 1024
        ),
        name="sage",
    )(*args)


def solution(mesh):
    placed = (
        P("dom", "mp"),
        P(None, "mp"),
        P(),
        P(None, "mp"),
        P(),
        P("dom", None, None),
        P("dom", None),
        P("dom"),
        P("dom"),
        P("dom", None),
        P("dom"),
        P("dom"),
    )
    return jax.shard_map(
        functools.partial(shards, mesh.shape["dom"]),
        mesh=mesh, in_specs=placed, out_specs=P("dom", "mp"), check_vma=False,
    )
```

```python
import functools

import jax
import jax.numpy as jnp
from jax import lax
from jax.experimental import pallas as pl
from jax.experimental.pallas import tpu as pltpu
from jax.sharding import PartitionSpec as P

MESH = pl.DeviceIdType.MESH
VMEM = pl.BlockSpec(memory_space=pltpu.VMEM)
ANY = pl.BlockSpec(memory_space=pl.ANY)
LANE = 128
TILE = 256
SPAN = 1024
DEPTH = 128


def bit(value, k):
    return lax.rem(lax.div(value, 2**k), 2)


def flips(me, n):
    return [2**k * (1 - 2 * bit(me, k)) for k in range((n - 1).bit_length())]


def exchanged(me, flip, mask):
    for k, delta in enumerate(flip):
        me = me + bit(mask, k) * delta
    return me


def mask_of(step, n, outer):
    half, quarter = n // 2, max(1, n // 4)

    def near(at):
        return at + quarter - lax.div(at, quarter) * (half - 1)

    at, odd = lax.div(step, 2), lax.rem(step, 2)
    mixed = (1 - odd) * (half + at) + odd * near(at)
    return jnp.where(outer, jnp.where(step < half - 1, near(step), step + 1), mixed)


def dot(a, b):
    return jnp.dot(a, b, preferred_element_type=jnp.float32)


def across(pieces):
    return jnp.concatenate(pieces, axis=1)


def index_rows(index, near_ref, ints_ref):
    fan, rows = near_ref.shape
    own, count = ints_ref[0], ints_ref[1]
    pieces = [jnp.where(count > j, near_ref[j : j + 1, :], -1) for j in range(fan)]
    pieces += [own, count, jnp.zeros((index.shape[1] - fan - 2, rows), jnp.int32)]
    index[...] = jnp.concatenate(pieces, axis=0).T


def build_picks(index_ref, fan, sum_pick, own_pick, inverse, scaled, first, last):
    chunks = sum_pick.shape[0]
    high = 16

    def one(at, carry):
        r0 = pl.multiple_of(at * high, high)
        index = index_ref[pl.ds(r0, high), :]
        lanes = [
            jnp.broadcast_to(index[:, j : j + 1], (high, LANE)).astype(jnp.int16)
            for j in range(fan + 1)
        ]
        count = jnp.broadcast_to(index[:, fan + 1 : fan + 2], (high, LANE)).astype(jnp.float32)
        inverse[pl.ds(r0, high), :] = 1.0 / count
        lane = lax.broadcasted_iota(jnp.int32, (high, LANE), 1)
        one_value, no_value = jnp.bfloat16(1.0), jnp.bfloat16(0.0)
        own_value = count.astype(jnp.bfloat16) if scaled else one_value
        for c in range(chunks):
            column = (lane + c * LANE).astype(jnp.int16)
            total = jnp.where(lanes[0] == column, one_value, no_value)
            for j in range(1, fan):
                total = total + jnp.where(lanes[j] == column, one_value, no_value)
            sum_pick[c, pl.ds(r0, high), :] = total
            own_pick[c, pl.ds(r0, high), :] = jnp.where(lanes[fan] == column, own_value, no_value)
        return carry

    lax.fori_loop(first, last, one, 0)


def main_kernel(
    n,
    asked_any, table_any, near_a_any, self_a_any, count_a_any, near_b_any, self_b_any, count_b_any,
    weight_a_any, bias_a_any, weight_b_any, bias_b_any,
    out_ref,
    asked, table, near_a, ints_a, near_b, ints_b, wa, wb, bias,
    wide, wanted, wanted_scalar, stage, found, index_a, index_b,
    fetched, sum_a, own_a, sum_b, own_b, inv_a, inv_b, mixed, total, hidden,
    ask_send, ask_recv, send_sem, recv_sem, relay_send, relay_recv, mp_send, mp_recv, load_sem, scalar_sem,
):
    me = lax.axis_index("dom")
    core = lax.axis_index("mp")
    partner = 1 - core
    flip = flips(me, n)
    cols, each = found.shape[1], found.shape[2]
    rows, seeds = inv_a.shape[0], inv_b.shape[0]
    feature, hidden_width = wa.shape[1] // 2, wb.shape[1] // 2
    fan_a, fan_b = near_a.shape[0], near_b.shape[0]
    blocks = wa.shape[0] // 2
    per = max(1, DEPTH // each)
    groups = n // per
    depth = per * each
    deep = depth // LANE
    mine = lax.div(me, per)
    outer = bit(me, max(0, len(flip) - 1)) == bit(me, max(0, len(flip) - 2))

    def peer(step):
        return exchanged(me, flip, mask_of(step, n, outer))

    own_blocks = pl.ds(core * blocks, blocks)
    loads = []
    for i, (target, sources) in enumerate([
        (near_a, [near_a_any]), (ints_a, [self_a_any, count_a_any]),
        (near_b, [near_b_any]), (ints_b, [self_b_any, count_b_any]), (asked, [asked_any]), (table, [table_any]),
        (bias, [bias_a_any, bias_b_any]),
        (wa.at[own_blocks], [weight_a_any.at[:, pl.ds(b * LANE, LANE)] for b in range(blocks)]),
        (wb.at[own_blocks], [weight_b_any.at[:, pl.ds(b * LANE, LANE)] for b in range(blocks)]),
    ]):
        if len(sources) == 1:
            pltpu.make_async_copy(sources[0], target, load_sem.at[i]).start()
        else:
            for b, source in enumerate(sources):
                pltpu.make_async_copy(source, target.at[b], load_sem.at[i]).start()
        loads.append(pltpu.make_async_copy(target, target, load_sem.at[i]))

    barrier = pltpu.get_barrier_semaphore()

    def greet(step, carry):
        pl.semaphore_signal(barrier, inc=1, device_id={"dom": peer(step)}, device_id_type=MESH)
        return carry

    lax.fori_loop(0, n - 1, greet, 0)
    pl.semaphore_signal(barrier, inc=1, device_id={"mp": partner}, device_id_type=MESH)

    loads[4].wait()
    wanted[me] = asked[me]
    pl.semaphore_wait(barrier, n)

    def ask(other):
        return pltpu.make_async_remote_copy(
            src_ref=asked.at[other], dst_ref=wanted.at[me],
            send_sem=ask_send, recv_sem=ask_recv.at[me],
            device_id={"dom": other}, device_id_type=MESH,
        )

    def give(other):
        return pltpu.make_async_remote_copy(
            src_ref=found.at[other], dst_ref=fetched.at[core, me],
            send_sem=send_sem, recv_sem=recv_sem.at[mine],
            device_id={"dom": other}, device_id_type=MESH,
        )

    def over(source, target, send, recv):
        return pltpu.make_async_remote_copy(
            src_ref=source, dst_ref=target, send_sem=send, recv_sem=recv,
            device_id={"mp": partner}, device_id_type=MESH,
        )

    def relay(group):
        landed = fetched.at[core, pl.ds(group * per, per)]
        return over(landed, landed, relay_send, relay_recv.at[group])

    def send_ask(step, carry):
        ask(peer(step)).start()
        return carry

    lax.fori_loop(0, n - 1, send_ask, 0)
    for load in loads[:4]:
        load.wait()
    index_rows(index_a, near_a, ints_a)
    index_rows(index_b, near_b, ints_b)
    steps = rows // 16
    first = steps // 8

    for load in loads[5:]:
        load.wait()
    shared = [
        over(w.at[own_blocks], w.at[own_blocks], mp_send.at[i], mp_recv.at[i]) for i, w in enumerate((wa, wb))
    ]
    for copy in shared:
        copy.start()

    def widen(tile, carry):
        at = pl.ds(pl.multiple_of(tile * 128, 128), 128)
        for c in range(cols):
            wide[c, at, :] = table[at, c * LANE : (c + 1) * LANE].astype(jnp.float32)
        return carry

    lax.fori_loop(0, table.shape[0] // 128, widen, 0)
    build_picks(index_a, fan_a, sum_a, own_a, inv_a, True, 0, first)

    def to_scalar(other, step):
        slot = scalar_sem.at[lax.rem(step, scalar_sem.shape[0])]
        return pltpu.make_async_copy(wanted.at[other], wanted_scalar.at[other], slot)

    def find(other):
        for k in range(each):
            row = wanted_scalar[other, 0, k]
            for c in range(cols):
                stage[c, k : k + 1, :] = wide[c, pl.ds(row, 1), :]
        for c in range(cols):
            found[other, c] = stage[c].astype(jnp.bfloat16)

    behind = scalar_sem.shape[0] - 1

    def step_peer(step):
        return exchanged(me, flip, jnp.where(step < n - 1, mask_of(step, n, outer), 0))

    def find_and_send(step, carry):
        @pl.when(step < n)
        def _():
            other = step_peer(step)

            @pl.when(step < n - 1)
            def _():
                pltpu.make_async_copy(asked.at[other], wanted.at[other], ask_recv.at[other]).wait()

            to_scalar(other, step).start()

        @pl.when(step >= behind)
        def _():
            other = step_peer(step - behind)
            to_scalar(other, step - behind).wait()
            find(other)

            @pl.when(step - behind < n - 1)
            def _():
                give(other).start()

        return carry

    lax.fori_loop(0, n + behind, find_and_send, 0)
    fetched[core, me] = found[me]
    build_picks(index_a, fan_a, sum_a, own_a, inv_a, True, first, steps)
    build_picks(index_b, fan_b, sum_b, own_b, inv_b, False, 0, seeds // 16)
    total[...] = jnp.zeros_like(total)
    for copy in shared:
        copy.wait()

    group_flip = flips(mine, groups)

    def group_of(k):
        return exchanged(mine, group_flip, k)

    def take(group):
        def arrived(count):
            pltpu.make_async_copy(
                found.at[pl.ds(0, count)], fetched.at[core, pl.ds(0, count)], recv_sem.at[group]
            ).wait()

        @pl.when(group != mine)
        def _():
            arrived(per)

        if per > 1:
            @pl.when(group == mine)
            def _():
                arrived(per - 1)

        relay(group).start()

    def use(group):
        relay(group).wait_recv()
        lines = across([
            fetched[h, pl.ds(group * per, per), c].reshape(depth, LANE) for h in range(2) for c in range(cols)
        ])
        for which in range(2):
            at = pl.ds(which * feature, feature)
            for b in range(0, 2 * blocks, 2):
                value = dot(lines, across([wa[b, at, :], wa[b + 1, at, :]])).astype(jnp.bfloat16)
                for i in range(2):
                    mixed[b + i, which * depth : (which + 1) * depth, :] = value[:, i * LANE : (i + 1) * LANE]

        def one_tile(tile, carry):
            at = pl.ds(pl.multiple_of(tile * SPAN, SPAN), SPAN)
            picks = across([p[group * deep + i, at, :] for p in (own_a, sum_a) for i in range(deep)])
            for b in range(blocks):
                total[b, at, :] += dot(picks, across([mixed[2 * b], mixed[2 * b + 1]]))
            return carry

        lax.fori_loop(0, rows // SPAN, one_tile, 0)

    def one_group(k, carry):
        @pl.when(k < groups)
        def _():
            take(group_of(k))

        @pl.when(k > 0)
        def _():
            use(group_of(k - 1))

        return carry

    lax.fori_loop(0, groups + 1, one_group, 0)

    def hide(tile, carry):
        at = pl.ds(pl.multiple_of(tile * TILE, TILE), TILE)
        inverse = inv_a[at, :]
        for b in range(blocks):
            for i in range(2):
                cut = slice((2 * b + i) * LANE, (2 * b + i + 1) * LANE)
                value = total[b, at, i * LANE : (i + 1) * LANE] * inverse + bias[0, :, cut]
                hidden[2 * b + i, at, :] = jnp.maximum(value, 0.0).astype(jnp.bfloat16)
        return carry

    lax.fori_loop(0, rows // TILE, hide, 0)

    hidden_all = across([hidden[b] for b in range(2 * blocks)])
    chunks_b = own_b.shape[0]
    own = dot(across([own_b[c] for c in range(chunks_b)]), hidden_all).astype(jnp.bfloat16)
    mean = dot(across([sum_b[c] for c in range(chunks_b)]), hidden_all)
    mean = (mean * across([inv_b[...]] * (2 * blocks))).astype(jnp.bfloat16)
    state = dot(own, across([wb[b, :hidden_width] for b in range(2 * blocks)]))
    state = state + dot(mean, across([wb[b, hidden_width:] for b in range(2 * blocks)]))
    state = jnp.maximum(state + bias[1], 0.0)
    squares = jnp.sum(state * state, axis=1, keepdims=True)
    scale = jnp.sqrt(jnp.float32(hidden_width)) / jnp.sqrt(squares + hidden_width)
    state = (state * scale).astype(out_ref.dtype)
    half = out_ref.shape[1]
    for c in range(2):
        @pl.when(core == c)
        def _():
            out_ref[...] = state[:, c * half : (c + 1) * half]

    others = pl.ds(0, n - 1)
    pltpu.make_async_copy(asked.at[others], wanted.at[others], ask_send).wait()
    pltpu.make_async_copy(found.at[others], fetched.at[core, others], send_sem).wait()
    pltpu.make_async_copy(fetched.at[core], fetched.at[partner], relay_send).wait()


def shards(
    n,
    table,
    weight_a,
    bias_a,
    weight_b,
    bias_b,
    requests,
    near_a,
    self_a,
    count_a,
    near_b,
    self_b,
    count_b,
):
    each = requests.shape[2]
    half, half_hidden = table.shape[1], weight_a.shape[1]
    rows, seeds, slots = near_a.shape[0], near_b.shape[0], n * each
    wide = -(-(near_a.shape[1] + 2) // 8) * 8
    bf16, f32 = jnp.bfloat16, jnp.float32
    cols, blocks = half // LANE, half_hidden // LANE
    per = max(1, DEPTH // each)
    depth, groups = per * each, n // per
    args = (
        requests[0][:, None, :], table,
        near_a.T, self_a[None, :], count_a[None, :], near_b.T, self_b[None, :], count_b[None, :],
        weight_a, bias_a[None, :], weight_b, bias_b[None, :],
    )
    return pl.pallas_call(
        functools.partial(main_kernel, n),
        out_shape=pltpu.VMEM((seeds, half_hidden), bf16),
        in_specs=[ANY] * len(args),
        out_specs=VMEM,
        scratch_shapes=[
            pltpu.VMEM(args[0].shape, jnp.int32),
            pltpu.VMEM(table.shape, bf16),
            pltpu.VMEM(args[2].shape, jnp.int32),
            pltpu.VMEM((2, 1, rows), jnp.int32),
            pltpu.VMEM(args[5].shape, jnp.int32),
            pltpu.VMEM((2, 1, seeds), jnp.int32),
            pltpu.VMEM((2 * blocks, weight_a.shape[0], LANE), bf16),
            pltpu.VMEM((2 * blocks, weight_b.shape[0], LANE), bf16),
            pltpu.VMEM((2, 1, bias_a.shape[0]), f32),
            pltpu.VMEM((cols, table.shape[0], LANE), f32),
            pltpu.VMEM((n, 1, each), jnp.int32),
            pltpu.SMEM((n, 1, each), jnp.int32),
            pltpu.VMEM((cols, each, LANE), f32),
            pltpu.VMEM((n, cols, each, LANE), bf16),
            pltpu.VMEM((rows, wide), jnp.int32),
            pltpu.VMEM((seeds, wide), jnp.int32),
            pltpu.VMEM((2, n, cols, each, LANE), bf16),
            pltpu.VMEM((slots // LANE, rows, LANE), bf16),
            pltpu.VMEM((slots // LANE, rows, LANE), bf16),
            pltpu.VMEM((rows // LANE, seeds, LANE), bf16),
            pltpu.VMEM((rows // LANE, seeds, LANE), bf16),
            pltpu.VMEM((rows, LANE), f32),
            pltpu.VMEM((seeds, LANE), f32),
            pltpu.VMEM((2 * blocks, 2 * depth, LANE), bf16),
            pltpu.VMEM((blocks, rows, 2 * LANE), f32),
            pltpu.VMEM((2 * blocks, rows, LANE), bf16),
            pltpu.SemaphoreType.DMA,
            pltpu.SemaphoreType.DMA((n,)),
            pltpu.SemaphoreType.DMA,
            pltpu.SemaphoreType.DMA((groups,)),
            pltpu.SemaphoreType.DMA,
            pltpu.SemaphoreType.DMA((groups,)),
            pltpu.SemaphoreType.DMA((2,)),
            pltpu.SemaphoreType.DMA((2,)),
            pltpu.SemaphoreType.DMA((9,)),
            pltpu.SemaphoreType.DMA((4,)),
        ],
        compiler_params=pltpu.CompilerParams(
            collective_id=0, has_side_effects=True, vmem_limit_bytes=60 * 1024 * 1024
        ),
        name="sage",
    )(*args)


def solution(mesh):
    placed = (
        P("dom", "mp"),
        P(None, "mp"),
        P(),
        P(None, "mp"),
        P(),
        P("dom", None, None),
        P("dom", None),
        P("dom"),
        P("dom"),
        P("dom", None),
        P("dom"),
        P("dom"),
    )
    return jax.shard_map(
        functools.partial(shards, mesh.shape["dom"]),
        mesh=mesh, in_specs=placed, out_specs=P("dom", "mp"), check_vma=False,
    )
```

```python
import functools

import jax
import jax.numpy as jnp
from jax import lax
from jax.experimental import pallas as pl
from jax.experimental.pallas import tpu as pltpu
from jax.sharding import PartitionSpec as P

MESH = pl.DeviceIdType.MESH
VMEM = pl.BlockSpec(memory_space=pltpu.VMEM)
ANY = pl.BlockSpec(memory_space=pl.ANY)
LANE = 128
TILE = 256
SPAN = 1024
PART = 4
DEPTH = 256


def bit(value, k):
    return lax.rem(lax.div(value, 2**k), 2)


def flips(me, n):
    return [2**k * (1 - 2 * bit(me, k)) for k in range((n - 1).bit_length())]


def exchanged(me, flip, mask):
    for k, delta in enumerate(flip):
        me = me + bit(mask, k) * delta
    return me


def mask_of(step, n):
    half, quarter = n // 2, n // 4
    crossing = half + quarter + lax.div(step, 2) - lax.rem(step, 2) * quarter
    return jnp.where(step < half, crossing, step - half + 1)


def dot(a, b):
    return jnp.dot(a, b, preferred_element_type=jnp.float32)


def across(pieces):
    return jnp.concatenate(pieces, axis=1)


def index_rows(index, near_ref, ints_ref):
    fan, rows = near_ref.shape
    own, count = ints_ref[0], ints_ref[1]
    pieces = [jnp.where(count > j, near_ref[j : j + 1, :], -1) for j in range(fan)]
    pieces += [own, count, jnp.zeros((index.shape[1] - fan - 2, rows), jnp.int32)]
    index[...] = jnp.concatenate(pieces, axis=0).T


def spread_matrix(width, fan):
    shape = (2 * width, (fan + 2) * LANE)
    line = lax.broadcasted_iota(jnp.int32, shape, 0)
    block = lax.broadcasted_iota(jnp.int32, shape, 1) >> 7
    high = jnp.where(line == block, 128.0, 0.0)
    return jnp.where(line == block + width, 1.0, high).astype(jnp.bfloat16)


def spread_index(index_ref, matrix, spread, inverse, weight):
    rows = index_ref.shape[0]
    fan = spread.shape[0] - 1
    size = min(rows, TILE)

    def one(at, carry):
        r0 = pl.ds(pl.multiple_of(at * size, size), size)
        index = index_ref[r0, :]
        parts = across([index >> 7, index & 127]).astype(jnp.float32).astype(jnp.bfloat16)
        for j in range(0, fan + 2, 2):
            wide = dot(parts, matrix[:, j * LANE : min(j + 2, fan + 2) * LANE])
            for i in range(min(2, fan + 2 - j)):
                value = wide[:, i * LANE : (i + 1) * LANE]
                if j + i <= fan:
                    spread[j + i, r0, :] = value.astype(jnp.int32)
                else:
                    inverse[r0, :] = 1.0 / value
                    if weight is not None:
                        weight[r0, :] = value
        return carry

    lax.fori_loop(0, rows // size, one, 0)


def build_picks(spread, weight, sum_pick, own_pick, start, chunks, base, first, last):
    fan = spread.shape[0] - 1
    high = 16

    def one(at, carry):
        for part in range(PART):
            r0 = pl.ds(pl.multiple_of((at * PART + part) * high, high), high)
            lanes = [spread[j, r0, :].astype(jnp.int16) for j in range(fan + 1)]
            lane = lax.broadcasted_iota(jnp.int32, (high, LANE), 1) + base
            one_value, no_value = jnp.bfloat16(1.0), jnp.bfloat16(0.0)
            own_value = one_value if weight is None else weight[r0, :].astype(jnp.bfloat16)
            for c in range(chunks):
                column = (lane + c * LANE).astype(jnp.int16)
                total = jnp.where(lanes[0] == column, one_value, no_value)
                for j in range(1, fan):
                    total = total + jnp.where(lanes[j] == column, one_value, no_value)
                sum_pick[start + c, r0, :] = total
                own_pick[start + c, r0, :] = jnp.where(lanes[fan] == column, own_value, no_value)
        return carry

    lax.fori_loop(first, last, one, 0)


def main_kernel(
    n,
    asked_any, table_any, near_a_any, self_a_any, count_a_any, near_b_any, self_b_any, count_b_any,
    weight_a_any, bias_a_any, weight_b_any, bias_b_any,
    out_ref,
    asked, table, near_a, ints_a, near_b, ints_b, wa, wb, bias,
    wide, wanted, wanted_scalar, stage, found, index_a, index_b,
    fetched, helped, near_h, ints_h, matrix_a, matrix_b, spread, spread_b, weight, sum_a, own_a, sum_h, own_h, sum_b, own_b,
    inv_a, inv_b, mixed, total, mixed_h, total_h, part_out, part_in, hidden,
    ask_send, ask_recv, send_sem, recv_sem, relay_send, relay_recv, mp_send, mp_recv, load_sem, scalar_sem,
    index_send, index_recv, help_recv, help_relay_send, help_relay_recv,
    part_send, part_recv, part_relay_send, part_relay_recv,
):
    me = lax.axis_index("dom")
    core = lax.axis_index("mp")
    partner = 1 - core
    flip = flips(me, n)
    cols, each = found.shape[1], found.shape[2]
    rows, seeds = inv_a.shape[0], inv_b.shape[0]
    feature, hidden_width = wa.shape[1] // 2, wb.shape[1] // 2
    fan_a, fan_b = near_a.shape[0], near_b.shape[0]
    blocks = wa.shape[0] // 2
    per = max(1, DEPTH // each)
    groups = n // per
    depth = per * each
    deep = depth // LANE
    mine = lax.div(me, per)
    half, half_groups = n // 2, groups // 2
    half_chunks = sum_a.shape[0] // 2
    outer = bit(me, len(flip) - 1) == bit(me, len(flip) - 2)
    inner = bit(me, len(flip) - 1) != bit(me, len(flip) - 2)
    twin = exchanged(me, flip, half + half // 2)
    here = lax.rem(me, half)
    near_base = bit(me, len(flip) - 1) * (half_chunks * LANE)
    far_base = half_chunks * LANE - near_base

    def peer(step):
        return exchanged(me, flip, mask_of(step, n))

    own_blocks = pl.ds(core * blocks, blocks)
    loads = []
    for i, (target, sources) in enumerate([
        (near_a, [near_a_any]), (ints_a, [self_a_any, count_a_any]),
        (near_b, [near_b_any]), (ints_b, [self_b_any, count_b_any]), (asked, [asked_any]), (table, [table_any]),
        (bias, [bias_a_any, bias_b_any]),
        (wa.at[own_blocks], [weight_a_any.at[:, pl.ds(b * LANE, LANE)] for b in range(blocks)]),
        (wb.at[own_blocks], [weight_b_any.at[:, pl.ds(b * LANE, LANE)] for b in range(blocks)]),
    ]):
        if len(sources) == 1:
            pltpu.make_async_copy(sources[0], target, load_sem.at[i]).start()
        else:
            for b, source in enumerate(sources):
                pltpu.make_async_copy(source, target.at[b], load_sem.at[i]).start()
        loads.append(pltpu.make_async_copy(target, target, load_sem.at[i]))

    barrier = pltpu.get_barrier_semaphore()

    def greet(step, carry):
        pl.semaphore_signal(barrier, inc=1, device_id={"dom": peer(step)}, device_id_type=MESH)
        return carry

    lax.fori_loop(0, n - 1, greet, 0)
    pl.semaphore_signal(barrier, inc=1, device_id={"mp": partner}, device_id_type=MESH)

    loads[4].wait()
    wanted[me] = asked[me]
    pl.semaphore_wait(barrier, n)

    def ask(other):
        return pltpu.make_async_remote_copy(
            src_ref=asked.at[other], dst_ref=wanted.at[me],
            send_sem=ask_send, recv_sem=ask_recv.at[me],
            device_id={"dom": other}, device_id_type=MESH,
        )

    def give(other):
        return pltpu.make_async_remote_copy(
            src_ref=found.at[other], dst_ref=fetched.at[core, me],
            send_sem=send_sem, recv_sem=recv_sem.at[mine],
            device_id={"dom": other}, device_id_type=MESH,
        )

    def lend(source, helper):
        return pltpu.make_async_remote_copy(
            src_ref=found.at[source], dst_ref=helped.at[core, here],
            send_sem=send_sem, recv_sem=help_recv.at[lax.div(here, per)],
            device_id={"dom": helper}, device_id_type=MESH,
        )

    def to_twin(source, target, send, recv):
        return pltpu.make_async_remote_copy(
            src_ref=source, dst_ref=target, send_sem=send, recv_sem=recv,
            device_id={"dom": twin}, device_id_type=MESH,
        )

    def over(source, target, send, recv):
        return pltpu.make_async_remote_copy(
            src_ref=source, dst_ref=target, send_sem=send, recv_sem=recv,
            device_id={"mp": partner}, device_id_type=MESH,
        )

    def relay(group):
        landed = fetched.at[core, pl.ds(group * per, per)]
        return over(landed, landed, relay_send, relay_recv.at[group])

    def send_ask(step, carry):
        ask(peer(step)).start()
        return carry

    lax.fori_loop(0, n - 1, send_ask, 0)
    for load in loads[:4]:
        load.wait()
    index_rows(index_b, near_b, ints_b)
    index_copies = [
        to_twin(near_a, near_h, index_send.at[0], index_recv.at[0]),
        to_twin(ints_a, ints_h, index_send.at[1], index_recv.at[1]),
    ]

    @pl.when(outer)
    def _():
        for copy in index_copies:
            copy.start()

    for load in loads[5:]:
        load.wait()
    shared = [
        over(w.at[own_blocks], w.at[own_blocks], mp_send.at[i], mp_recv.at[i]) for i, w in enumerate((wa, wb))
    ]
    for copy in shared:
        copy.start()

    def widen(tile, carry):
        at = pl.ds(pl.multiple_of(tile * 128, 128), 128)
        for c in range(cols):
            wide[c, at, :] = table[at, c * LANE : (c + 1) * LANE].astype(jnp.float32)
        return carry

    lax.fori_loop(0, table.shape[0] // 128, widen, 0)
    matrix_a[...] = spread_matrix(index_a.shape[1], fan_a)
    matrix_b[...] = spread_matrix(index_b.shape[1], fan_b)
    steps = rows // (16 * PART)

    def to_scalar(other, step):
        slot = scalar_sem.at[lax.rem(step, scalar_sem.shape[0])]
        return pltpu.make_async_copy(wanted.at[other], wanted_scalar.at[other], slot)

    def find(other):
        for k in range(each):
            row = wanted_scalar[other, 0, k]
            for c in range(cols):
                stage[c, k : k + 1, :] = wide[c, pl.ds(row, 1), :]
        for c in range(cols):
            found[other, c] = stage[c].astype(jnp.bfloat16)

    behind = scalar_sem.shape[0] - 1

    def step_peer(step):
        return exchanged(me, flip, jnp.where(step < n - 1, mask_of(step, n), 0))

    def find_and_send(step, carry):
        @pl.when(step < n)
        def _():
            other = step_peer(step)

            @pl.when(step < n - 1)
            def _():
                pltpu.make_async_copy(asked.at[other], wanted.at[other], ask_recv.at[other]).wait()

            to_scalar(other, step).start()

        @pl.when(step >= behind)
        def _():
            other = step_peer(step - behind)
            to_scalar(other, step - behind).wait()
            find(other)

            mask = mask_of(step - behind, n)
            low = half + jnp.where(outer, half // 2, 0)
            lent = (mask >= low) & (mask < low + half // 2)

            hop = mask - low + jnp.where(outer, 0, half // 2)

            @pl.when((step - behind < half) & lent & (hop == 0))
            def _():
                helped[core, here] = found[other]

            @pl.when((step - behind < half) & lent & (hop != 0))
            def _():
                lend(other, exchanged(me, flip, hop)).start()

            @pl.when((step - behind < half) & jnp.logical_not(lent))
            def _():
                give(other).start()

        return carry

    def give_near(mask, carry):
        give(exchanged(me, flip, mask)).start()
        return carry

    lax.fori_loop(0, n + behind, find_and_send, 0)
    fetched[core, me] = found[me]

    for copy in shared:
        copy.wait()

    group_flip = flips(mine, groups)

    def turn_of(k):
        quarter = groups // 4
        turned = (3 - lax.div(k, quarter)) * quarter + lax.rem(k, quarter)
        return jnp.where(outer, k, turned)

    def group_of(k):
        return exchanged(mine, group_flip, turn_of(k))

    def arrived(count, sem):
        pltpu.make_async_copy(found.at[pl.ds(0, count)], fetched.at[core, pl.ds(0, count)], sem).wait()

    def take(group):
        @pl.when(group != mine)
        def _():
            arrived(per, recv_sem.at[group])

        if per > 1:
            @pl.when(group == mine)
            def _():
                arrived(per - 1, recv_sem.at[group])

        relay(group).start()

    def use(group, chunk):
        relay(group).wait_recv()
        lines = across([
            fetched[h, pl.ds(group * per, per), c].reshape(depth, LANE) for h in range(2) for c in range(cols)
        ])
        for which in range(2):
            at = pl.ds(which * feature, feature)
            for b in range(0, 2 * blocks, 2):
                value = dot(lines, across([wa[b, at, :], wa[b + 1, at, :]])).astype(jnp.bfloat16)
                for i in range(2):
                    mixed[b + i, which * depth : (which + 1) * depth, :] = value[:, i * LANE : (i + 1) * LANE]

        def one_tile(tile, carry):
            at = pl.ds(pl.multiple_of(tile * SPAN, SPAN), SPAN)
            picks = across([p[chunk + i, at, :] for p in (own_a, sum_a) for i in range(deep)])
            for b in range(blocks):
                total[b, at, :] += dot(picks, across([mixed[2 * b], mixed[2 * b + 1]]))
            return carry

        lax.fori_loop(0, rows // SPAN, one_tile, 0)

    def help_relay(group):
        landed = helped.at[core, pl.ds(group * per, per)]
        return over(landed, landed, help_relay_send, help_relay_recv.at[group])

    def help_take(group):
        @pl.when(group != lax.div(here, per))
        def _():
            arrived(per, help_recv.at[group])

        if per > 1:
            @pl.when(group == lax.div(here, per))
            def _():
                arrived(per - 1, help_recv.at[group])

        help_relay(group).start()

    def help_use(group):
        help_relay(group).wait_recv()
        lines = across([
            helped[h, pl.ds(group * per, per), c].reshape(depth, LANE) for h in range(2) for c in range(cols)
        ])
        for which in range(2):
            at = pl.ds(which * feature, feature)
            value = dot(lines, across([wa[core * blocks + i, at, :] for i in range(blocks)])).astype(jnp.bfloat16)
            for i in range(blocks):
                mixed_h[i, which * depth : (which + 1) * depth, :] = value[:, i * LANE : (i + 1) * LANE]

        def one_tile(tile, carry):
            at = pl.ds(pl.multiple_of(tile * SPAN, SPAN), SPAN)
            picks = across([p[group * deep + i, at, :] for p in (own_h, sum_h) for i in range(deep)])
            total_h[at, :] += dot(picks, across([mixed_h[i] for i in range(blocks)]))
            return carry

        lax.fori_loop(0, rows // SPAN, one_tile, 0)

    tiles = rows // TILE

    def part_copy(tile):
        return to_twin(
            part_out.at[tile], part_in.at[core, tile], part_send, part_recv.at[tile]
        )

    def part_relay(tile):
        landed = part_in.at[core, tile]
        return over(landed, landed, part_relay_send, part_relay_recv.at[tile])

    @pl.when(outer)
    def _():
        for copy in index_copies:
            copy.wait_recv()
        index_rows(index_a, near_h, ints_h)
        total_h[...] = jnp.zeros_like(total_h)
        spread_index(index_a, matrix_a, spread, inv_a, weight)
        build_picks(spread, weight, sum_h, own_h, 0, half_chunks, near_base, 0, steps)
        lax.fori_loop(1, half, give_near, 0)

        def one_help(k, carry):
            @pl.when(k < half_groups)
            def _():
                help_take(k)

            @pl.when(k > 0)
            def _():
                help_use(k - 1)

            return carry

        lax.fori_loop(0, half_groups + 1, one_help, 0)

        def put(tile, carry):
            at = pl.ds(pl.multiple_of(tile * TILE, TILE), TILE)
            for i in range(blocks):
                part_out[tile, i] = total_h[at, i * LANE : (i + 1) * LANE].astype(jnp.bfloat16)
            part_copy(tile).start()
            return carry

        lax.fori_loop(0, tiles, put, 0)

    index_rows(index_a, near_a, ints_a)
    spread_index(index_a, matrix_a, spread, inv_a, weight)
    build_picks(spread, weight, sum_a, own_a, 0, half_chunks, near_base, 0, steps)

    @pl.when(inner)
    def _():
        lax.fori_loop(1, half, give_near, 0)
        build_picks(spread, weight, sum_a, own_a, half_chunks, half_chunks, far_base, 0, steps)

    spread_index(index_b, matrix_b, spread_b, inv_b, None)
    build_picks(spread_b, None, sum_b, own_b, 0, own_b.shape[0], 0, 0, seeds // (16 * PART))
    total[...] = jnp.zeros_like(total)
    live_groups = jnp.where(outer, half_groups, groups)

    def one_group(k, carry):
        @pl.when(k < live_groups)
        def _():
            take(group_of(k))

        @pl.when(k > 0)
        def _():
            group = group_of(k - 1)
            far = lax.div(turn_of(k - 1), half_groups)
            use(group, (lax.rem(group, half_groups) + far * half_groups) * deep)

        return carry

    lax.fori_loop(0, live_groups + 1, one_group, 0)

    def hide(tile, parts):
        at = pl.ds(pl.multiple_of(tile * TILE, TILE), TILE)
        inverse = inv_a[at, :]
        for b in range(2 * blocks):
            value = total[b // 2, at, (b % 2) * LANE : (b % 2 + 1) * LANE]
            if parts:
                value = value + part_in[b // blocks, tile, b % blocks].astype(jnp.float32)
            value = value * inverse + bias[0, :, b * LANE : (b + 1) * LANE]
            hidden[b, at, :] = jnp.maximum(value, 0.0).astype(jnp.bfloat16)

    @pl.when(inner)
    def _():
        def plain(tile, carry):
            hide(tile, False)
            return carry

        lax.fori_loop(0, tiles, plain, 0)

    @pl.when(outer)
    def _():
        def pass_on(tile, carry):
            part_copy(tile).wait_recv()
            part_relay(tile).start()
            return carry

        def joined(tile, carry):
            part_relay(tile).wait_recv()
            hide(tile, True)
            return carry

        lax.fori_loop(0, tiles, pass_on, 0)
        lax.fori_loop(0, tiles, joined, 0)

    hidden_all = across([hidden[b] for b in range(2 * blocks)])
    chunks_b = own_b.shape[0]
    own = dot(across([own_b[c] for c in range(chunks_b)]), hidden_all).astype(jnp.bfloat16)
    mean = dot(across([sum_b[c] for c in range(chunks_b)]), hidden_all)
    mean = (mean * across([inv_b[...]] * (2 * blocks))).astype(jnp.bfloat16)
    state = dot(own, across([wb[b, :hidden_width] for b in range(2 * blocks)]))
    state = state + dot(mean, across([wb[b, hidden_width:] for b in range(2 * blocks)]))
    state = jnp.maximum(state + bias[1], 0.0)
    squares = jnp.sum(state * state, axis=1, keepdims=True)
    scale = jnp.sqrt(jnp.float32(hidden_width)) / jnp.sqrt(squares + hidden_width)
    state = (state * scale).astype(out_ref.dtype)
    width = out_ref.shape[1]
    for c in range(2):
        @pl.when(core == c)
        def _():
            out_ref[...] = state[:, c * width : (c + 1) * width]

    others = pl.ds(0, n - 1)
    pltpu.make_async_copy(asked.at[others], wanted.at[others], ask_send).wait()

    @pl.when(outer)
    def _():
        for copy in index_copies:
            copy.wait_send()
        arrived(n - 2, send_sem)
        arrived(half, relay_send)
        arrived(half, help_relay_send)
        pltpu.make_async_copy(part_out, part_in.at[core], part_send).wait()
        pltpu.make_async_copy(part_in.at[core], part_in.at[partner], part_relay_send).wait()

    @pl.when(inner)
    def _():
        arrived(n - 1, send_sem)
        arrived(n, relay_send)


def shards(
    n,
    table,
    weight_a,
    bias_a,
    weight_b,
    bias_b,
    requests,
    near_a,
    self_a,
    count_a,
    near_b,
    self_b,
    count_b,
):
    each = requests.shape[2]
    half, half_hidden = table.shape[1], weight_a.shape[1]
    rows, seeds, slots = near_a.shape[0], near_b.shape[0], n * each
    wide = -(-(near_a.shape[1] + 2) // 8) * 8
    bf16, f32 = jnp.bfloat16, jnp.float32
    cols, blocks = half // LANE, half_hidden // LANE
    per = max(1, DEPTH // each)
    depth, groups = per * each, n // per
    args = (
        requests[0][:, None, :], table,
        near_a.T, self_a[None, :], count_a[None, :], near_b.T, self_b[None, :], count_b[None, :],
        weight_a, bias_a[None, :], weight_b, bias_b[None, :],
    )
    return pl.pallas_call(
        functools.partial(main_kernel, n),
        out_shape=pltpu.VMEM((seeds, half_hidden), bf16),
        in_specs=[ANY] * len(args),
        out_specs=VMEM,
        scratch_shapes=[
            pltpu.VMEM(args[0].shape, jnp.int32),
            pltpu.VMEM(table.shape, bf16),
            pltpu.VMEM(args[2].shape, jnp.int32),
            pltpu.VMEM((2, 1, rows), jnp.int32),
            pltpu.VMEM(args[5].shape, jnp.int32),
            pltpu.VMEM((2, 1, seeds), jnp.int32),
            pltpu.VMEM((2 * blocks, weight_a.shape[0], LANE), bf16),
            pltpu.VMEM((2 * blocks, weight_b.shape[0], LANE), bf16),
            pltpu.VMEM((2, 1, bias_a.shape[0]), f32),
            pltpu.VMEM((cols, table.shape[0], LANE), f32),
            pltpu.VMEM((n, 1, each), jnp.int32),
            pltpu.SMEM((n, 1, each), jnp.int32),
            pltpu.VMEM((cols, each, LANE), f32),
            pltpu.VMEM((n, cols, each, LANE), bf16),
            pltpu.VMEM((rows, wide), jnp.int32),
            pltpu.VMEM((seeds, wide), jnp.int32),
            pltpu.VMEM((2, n, cols, each, LANE), bf16),
            pltpu.VMEM((2, n // 2, cols, each, LANE), bf16),
            pltpu.VMEM(args[2].shape, jnp.int32),
            pltpu.VMEM((2, 1, rows), jnp.int32),
            pltpu.VMEM((2 * wide, (near_a.shape[1] + 2) * LANE), bf16),
            pltpu.VMEM((2 * wide, (near_b.shape[1] + 2) * LANE), bf16),
            pltpu.VMEM((near_a.shape[1] + 1, rows, LANE), jnp.int32),
            pltpu.VMEM((near_b.shape[1] + 1, seeds, LANE), jnp.int32),
            pltpu.VMEM((rows, LANE), f32),
            pltpu.VMEM((slots // LANE, rows, LANE), bf16),
            pltpu.VMEM((slots // LANE, rows, LANE), bf16),
            pltpu.VMEM((slots // LANE // 2, rows, LANE), bf16),
            pltpu.VMEM((slots // LANE // 2, rows, LANE), bf16),
            pltpu.VMEM((rows // LANE, seeds, LANE), bf16),
            pltpu.VMEM((rows // LANE, seeds, LANE), bf16),
            pltpu.VMEM((rows, LANE), f32),
            pltpu.VMEM((seeds, LANE), f32),
            pltpu.VMEM((2 * blocks, 2 * depth, LANE), bf16),
            pltpu.VMEM((blocks, rows, 2 * LANE), f32),
            pltpu.VMEM((blocks, 2 * depth, LANE), bf16),
            pltpu.VMEM((rows, half_hidden), f32),
            pltpu.VMEM((rows // TILE, blocks, TILE, LANE), bf16),
            pltpu.VMEM((2, rows // TILE, blocks, TILE, LANE), bf16),
            pltpu.VMEM((2 * blocks, rows, LANE), bf16),
            pltpu.SemaphoreType.DMA,
            pltpu.SemaphoreType.DMA((n,)),
            pltpu.SemaphoreType.DMA,
            pltpu.SemaphoreType.DMA((groups,)),
            pltpu.SemaphoreType.DMA,
            pltpu.SemaphoreType.DMA((groups,)),
            pltpu.SemaphoreType.DMA((2,)),
            pltpu.SemaphoreType.DMA((2,)),
            pltpu.SemaphoreType.DMA((9,)),
            pltpu.SemaphoreType.DMA((4,)),
            pltpu.SemaphoreType.DMA((2,)),
            pltpu.SemaphoreType.DMA((2,)),
            pltpu.SemaphoreType.DMA((groups // 2,)),
            pltpu.SemaphoreType.DMA,
            pltpu.SemaphoreType.DMA((groups // 2,)),
            pltpu.SemaphoreType.DMA,
            pltpu.SemaphoreType.DMA((rows // TILE,)),
            pltpu.SemaphoreType.DMA,
            pltpu.SemaphoreType.DMA((rows // TILE,)),
        ],
        compiler_params=pltpu.CompilerParams(
            collective_id=0, has_side_effects=True, vmem_limit_bytes=60 * 1024 * 1024
        ),
        name="sage",
    )(*args)


def solution(mesh):
    placed = (
        P("dom", "mp"),
        P(None, "mp"),
        P(),
        P(None, "mp"),
        P(),
        P("dom", None, None),
        P("dom", None),
        P("dom"),
        P("dom"),
        P("dom", None),
        P("dom"),
        P("dom"),
    )
    return jax.shard_map(
        functools.partial(shards, mesh.shape["dom"]),
        mesh=mesh, in_specs=placed, out_specs=P("dom", "mp"), check_vma=False,
    )
```

```python
import functools

import jax
import jax.numpy as jnp
from jax import lax
from jax.experimental import pallas as pl
from jax.experimental.pallas import tpu as pltpu
from jax.sharding import PartitionSpec as P

MESH = pl.DeviceIdType.MESH
VMEM = pl.BlockSpec(memory_space=pltpu.VMEM)
ANY = pl.BlockSpec(memory_space=pl.ANY)
LANE = 128
TILE = 256
SPAN = 1024
PART = 4
DEPTH = 256


def bit(value, k):
    return lax.rem(lax.div(value, 2**k), 2)


def flips(me, n):
    return [2**k * (1 - 2 * bit(me, k)) for k in range((n - 1).bit_length())]


def exchanged(me, flip, mask):
    for k, delta in enumerate(flip):
        me = me + bit(mask, k) * delta
    return me


def mask_of(step, n, outer):
    half, quarter = n // 2, n // 4
    odd = lax.rem(step, 2)
    first = half + quarter + lax.div(step, 2) - odd * jnp.where(outer, half, quarter)
    at = step - half
    crossing = jnp.where(at < quarter, half + at, at - quarter + 1)
    return jnp.where(step < half, first, jnp.where(outer, crossing, at + 1))


def dot(a, b):
    return jnp.dot(a, b, preferred_element_type=jnp.float32)


def across(pieces):
    return jnp.concatenate(pieces, axis=1)


def index_rows(index, near_ref, ints_ref):
    fan, rows = near_ref.shape
    own, count = ints_ref[0], ints_ref[1]
    pieces = [jnp.where(count > j, near_ref[j : j + 1, :], -1) for j in range(fan)]
    pieces += [own, count, jnp.zeros((index.shape[1] - fan - 2, rows), jnp.int32)]
    index[...] = jnp.concatenate(pieces, axis=0).T


def spread_matrix(width, fan):
    shape = (2 * width, (fan + 2) * LANE)
    line = lax.broadcasted_iota(jnp.int32, shape, 0)
    block = lax.broadcasted_iota(jnp.int32, shape, 1) >> 7
    high = jnp.where(line == block, 128.0, 0.0)
    return jnp.where(line == block + width, 1.0, high).astype(jnp.bfloat16)


def spread_index(index_ref, matrix, spread, inverse, weight):
    rows = index_ref.shape[0]
    fan = spread.shape[0] - 1
    size = min(rows, TILE)

    def one(at, carry):
        r0 = pl.ds(pl.multiple_of(at * size, size), size)
        index = index_ref[r0, :]
        parts = across([index >> 7, index & 127]).astype(jnp.float32).astype(jnp.bfloat16)
        for j in range(0, fan + 2, 2):
            wide = dot(parts, matrix[:, j * LANE : min(j + 2, fan + 2) * LANE])
            for i in range(min(2, fan + 2 - j)):
                value = wide[:, i * LANE : (i + 1) * LANE]
                if j + i <= fan:
                    spread[j + i, r0, :] = value.astype(jnp.int32)
                else:
                    inverse[r0, :] = 1.0 / value
                    if weight is not None:
                        weight[r0, :] = value
        return carry

    lax.fori_loop(0, rows // size, one, 0)


def build_picks(spread, weight, sum_pick, own_pick, start, chunks, base, first, last):
    fan = spread.shape[0] - 1
    high = 16

    def one(at, carry):
        for part in range(PART):
            r0 = pl.ds(pl.multiple_of((at * PART + part) * high, high), high)
            lanes = [spread[j, r0, :].astype(jnp.int16) for j in range(fan + 1)]
            lane = lax.broadcasted_iota(jnp.int32, (high, LANE), 1) + base
            one_value, no_value = jnp.bfloat16(1.0), jnp.bfloat16(0.0)
            own_value = one_value if weight is None else weight[r0, :].astype(jnp.bfloat16)
            for c in range(chunks):
                column = (lane + c * LANE).astype(jnp.int16)
                total = jnp.where(lanes[0] == column, one_value, no_value)
                for j in range(1, fan):
                    total = total + jnp.where(lanes[j] == column, one_value, no_value)
                sum_pick[start + c, r0, :] = total
                own_pick[start + c, r0, :] = jnp.where(lanes[fan] == column, own_value, no_value)
        return carry

    lax.fori_loop(first, last, one, 0)


def main_kernel(
    n,
    asked_any, table_any, near_a_any, self_a_any, count_a_any, near_b_any, self_b_any, count_b_any,
    weight_a_any, bias_a_any, weight_b_any, bias_b_any,
    out_ref,
    asked, table, near_a, ints_a, near_b, ints_b, wa, wb, bias,
    wide, wanted, wanted_scalar, stage, found, index_a, index_b,
    fetched, helped, near_h, ints_h, matrix_a, matrix_b, spread, spread_b, weight, sum_a, own_a, sum_h, own_h, sum_b, own_b,
    inv_a, inv_b, mixed, total, mixed_h, total_h, part_out, part_in, hidden,
    ask_send, ask_recv, send_sem, recv_sem, relay_send, relay_recv, mp_send, mp_recv, load_sem, scalar_sem,
    index_send, index_recv, help_recv, help_relay_send, help_relay_recv,
    part_send, part_recv, part_relay_send, part_relay_recv,
):
    me = lax.axis_index("dom")
    core = lax.axis_index("mp")
    partner = 1 - core
    flip = flips(me, n)
    cols, each = found.shape[1], found.shape[2]
    rows, seeds = inv_a.shape[0], inv_b.shape[0]
    feature, hidden_width = wa.shape[1] // 2, wb.shape[1] // 2
    fan_a, fan_b = near_a.shape[0], near_b.shape[0]
    blocks = wa.shape[0] // 2
    per = max(1, DEPTH // each)
    groups = n // per
    depth = per * each
    deep = depth // LANE
    mine = lax.div(me, per)
    half, half_groups = n // 2, groups // 2
    half_chunks = sum_a.shape[0] // 2
    outer = bit(me, len(flip) - 1) == bit(me, len(flip) - 2)
    inner = bit(me, len(flip) - 1) != bit(me, len(flip) - 2)
    twin = exchanged(me, flip, half + half // 2)
    here = lax.rem(me, half)
    near_base = bit(me, len(flip) - 1) * (half_chunks * LANE)
    far_base = half_chunks * LANE - near_base

    def peer(step):
        return exchanged(me, flip, mask_of(step, n, outer))

    own_blocks = pl.ds(core * blocks, blocks)
    loads = []
    for i, (target, sources) in enumerate([
        (near_a, [near_a_any]), (ints_a, [self_a_any, count_a_any]),
        (near_b, [near_b_any]), (ints_b, [self_b_any, count_b_any]), (asked, [asked_any]), (table, [table_any]),
        (bias, [bias_a_any, bias_b_any]),
        (wa.at[own_blocks], [weight_a_any.at[:, pl.ds(b * LANE, LANE)] for b in range(blocks)]),
        (wb.at[own_blocks], [weight_b_any.at[:, pl.ds(b * LANE, LANE)] for b in range(blocks)]),
    ]):
        if len(sources) == 1:
            pltpu.make_async_copy(sources[0], target, load_sem.at[i]).start()
        else:
            for b, source in enumerate(sources):
                pltpu.make_async_copy(source, target.at[b], load_sem.at[i]).start()
        loads.append(pltpu.make_async_copy(target, target, load_sem.at[i]))

    barrier = pltpu.get_barrier_semaphore()

    def greet(step, carry):
        pl.semaphore_signal(barrier, inc=1, device_id={"dom": peer(step)}, device_id_type=MESH)
        return carry

    lax.fori_loop(0, n - 1, greet, 0)
    pl.semaphore_signal(barrier, inc=1, device_id={"mp": partner}, device_id_type=MESH)

    loads[4].wait()
    wanted[me] = asked[me]
    pl.semaphore_wait(barrier, n)

    def ask(other):
        return pltpu.make_async_remote_copy(
            src_ref=asked.at[other], dst_ref=wanted.at[me],
            send_sem=ask_send, recv_sem=ask_recv.at[me],
            device_id={"dom": other}, device_id_type=MESH,
        )

    def give(other):
        return pltpu.make_async_remote_copy(
            src_ref=found.at[other], dst_ref=fetched.at[core, me],
            send_sem=send_sem, recv_sem=recv_sem.at[mine],
            device_id={"dom": other}, device_id_type=MESH,
        )

    def lend(source, helper):
        return pltpu.make_async_remote_copy(
            src_ref=found.at[source], dst_ref=helped.at[core, here],
            send_sem=send_sem, recv_sem=help_recv.at[lax.div(here, per)],
            device_id={"dom": helper}, device_id_type=MESH,
        )

    def to_twin(source, target, send, recv):
        return pltpu.make_async_remote_copy(
            src_ref=source, dst_ref=target, send_sem=send, recv_sem=recv,
            device_id={"dom": twin}, device_id_type=MESH,
        )

    def over(source, target, send, recv):
        return pltpu.make_async_remote_copy(
            src_ref=source, dst_ref=target, send_sem=send, recv_sem=recv,
            device_id={"mp": partner}, device_id_type=MESH,
        )

    def relay(group):
        landed = fetched.at[core, pl.ds(group * per, per)]
        return over(landed, landed, relay_send, relay_recv.at[group])

    def send_ask(step, carry):
        ask(peer(step)).start()
        return carry

    lax.fori_loop(0, n - 1, send_ask, 0)
    for load in loads[:4]:
        load.wait()
    index_rows(index_b, near_b, ints_b)
    index_copies = [
        to_twin(near_a, near_h, index_send.at[0], index_recv.at[0]),
        to_twin(ints_a, ints_h, index_send.at[1], index_recv.at[1]),
    ]

    @pl.when(outer)
    def _():
        for copy in index_copies:
            copy.start()

    for load in loads[5:]:
        load.wait()
    shared = [
        over(w.at[own_blocks], w.at[own_blocks], mp_send.at[i], mp_recv.at[i]) for i, w in enumerate((wa, wb))
    ]
    for copy in shared:
        copy.start()

    def widen(tile, carry):
        at = pl.ds(pl.multiple_of(tile * 128, 128), 128)
        for c in range(cols):
            wide[c, at, :] = table[at, c * LANE : (c + 1) * LANE].astype(jnp.float32)
        return carry

    lax.fori_loop(0, table.shape[0] // 128, widen, 0)
    matrix_a[...] = spread_matrix(index_a.shape[1], fan_a)
    matrix_b[...] = spread_matrix(index_b.shape[1], fan_b)
    steps = rows // (16 * PART)

    def to_scalar(other, step):
        slot = scalar_sem.at[lax.rem(step, scalar_sem.shape[0])]
        return pltpu.make_async_copy(wanted.at[other], wanted_scalar.at[other], slot)

    def find(other):
        for k in range(each):
            row = wanted_scalar[other, 0, k]
            for c in range(cols):
                stage[c, k : k + 1, :] = wide[c, pl.ds(row, 1), :]
        for c in range(cols):
            found[other, c] = stage[c].astype(jnp.bfloat16)

    behind = scalar_sem.shape[0] - 1

    def step_peer(step):
        return exchanged(me, flip, jnp.where(step < n - 1, mask_of(step, n, outer), 0))

    def find_and_send(step, carry):
        @pl.when(step < n)
        def _():
            other = step_peer(step)

            @pl.when(step < n - 1)
            def _():
                pltpu.make_async_copy(asked.at[other], wanted.at[other], ask_recv.at[other]).wait()

            to_scalar(other, step).start()

        @pl.when(step >= behind)
        def _():
            other = step_peer(step - behind)
            to_scalar(other, step - behind).wait()
            find(other)

            mask = mask_of(step - behind, n, outer)
            low = half + jnp.where(outer, half // 2, 0)
            lent = (mask >= low) & (mask < low + half // 2)

            hop = mask - low + jnp.where(outer, 0, half // 2)

            @pl.when((step - behind < half) & lent & (hop == 0))
            def _():
                helped[core, here] = found[other]

            @pl.when((step - behind < half) & lent & (hop != 0))
            def _():
                lend(other, exchanged(me, flip, hop)).start()

            @pl.when((step - behind < half + jnp.where(outer, half // 2, 0)) & jnp.logical_not(lent))
            def _():
                give(other).start()

        return carry

    def give_near(mask, carry):
        give(exchanged(me, flip, mask)).start()
        return carry

    lax.fori_loop(0, n + behind, find_and_send, 0)
    fetched[core, me] = found[me]

    for copy in shared:
        copy.wait()

    group_flip = flips(mine, groups)

    def turn_of(k):
        quarter = groups // 4
        turned = (3 - lax.div(k, quarter)) * quarter + lax.rem(k, quarter)
        return jnp.where(outer, k, turned)

    def group_of(k):
        return exchanged(mine, group_flip, turn_of(k))

    def arrived(count, sem):
        pltpu.make_async_copy(found.at[pl.ds(0, count)], fetched.at[core, pl.ds(0, count)], sem).wait()

    def take(group):
        @pl.when(group != mine)
        def _():
            arrived(per, recv_sem.at[group])

        if per > 1:
            @pl.when(group == mine)
            def _():
                arrived(per - 1, recv_sem.at[group])

        relay(group).start()

    def use(group, chunk):
        relay(group).wait_recv()
        lines = across([
            fetched[h, pl.ds(group * per, per), c].reshape(depth, LANE) for h in range(2) for c in range(cols)
        ])
        for which in range(2):
            at = pl.ds(which * feature, feature)
            for b in range(0, 2 * blocks, 2):
                value = dot(lines, across([wa[b, at, :], wa[b + 1, at, :]])).astype(jnp.bfloat16)
                for i in range(2):
                    mixed[b + i, which * depth : (which + 1) * depth, :] = value[:, i * LANE : (i + 1) * LANE]

        def one_tile(tile, carry):
            at = pl.ds(pl.multiple_of(tile * SPAN, SPAN), SPAN)
            picks = across([p[chunk + i, at, :] for p in (own_a, sum_a) for i in range(deep)])
            for b in range(blocks):
                total[b, at, :] += dot(picks, across([mixed[2 * b], mixed[2 * b + 1]]))
            return carry

        lax.fori_loop(0, rows // SPAN, one_tile, 0)

    def help_relay(group):
        landed = helped.at[core, pl.ds(group * per, per)]
        return over(landed, landed, help_relay_send, help_relay_recv.at[group])

    def help_take(group):
        @pl.when(group != lax.div(here, per))
        def _():
            arrived(per, help_recv.at[group])

        if per > 1:
            @pl.when(group == lax.div(here, per))
            def _():
                arrived(per - 1, help_recv.at[group])

        help_relay(group).start()

    def help_use(group):
        help_relay(group).wait_recv()
        lines = across([
            helped[h, pl.ds(group * per, per), c].reshape(depth, LANE) for h in range(2) for c in range(cols)
        ])
        for which in range(2):
            at = pl.ds(which * feature, feature)
            value = dot(lines, across([wa[core * blocks + i, at, :] for i in range(blocks)])).astype(jnp.bfloat16)
            for i in range(blocks):
                mixed_h[i, which * depth : (which + 1) * depth, :] = value[:, i * LANE : (i + 1) * LANE]

        def one_tile(tile, carry):
            at = pl.ds(pl.multiple_of(tile * SPAN, SPAN), SPAN)
            picks = across([p[group * deep + i, at, :] for p in (own_h, sum_h) for i in range(deep)])
            total_h[at, :] += dot(picks, across([mixed_h[i] for i in range(blocks)]))
            return carry

        lax.fori_loop(0, rows // SPAN, one_tile, 0)

    tiles = rows // TILE

    def part_copy(tile):
        return to_twin(
            part_out.at[tile], part_in.at[core, tile], part_send, part_recv.at[tile]
        )

    def part_relay(tile):
        landed = part_in.at[core, tile]
        return over(landed, landed, part_relay_send, part_relay_recv.at[tile])

    @pl.when(outer)
    def _():
        for copy in index_copies:
            copy.wait_recv()
        index_rows(index_a, near_h, ints_h)
        total_h[...] = jnp.zeros_like(total_h)
        spread_index(index_a, matrix_a, spread, inv_a, weight)
        build_picks(spread, weight, sum_h, own_h, 0, half_chunks, near_base, 0, steps)
        lax.fori_loop(1, half // 2, give_near, 0)

        def one_help(k, carry):
            @pl.when(k < half_groups)
            def _():
                help_take(k)

            @pl.when(k > 0)
            def _():
                help_use(k - 1)

            return carry

        lax.fori_loop(0, half_groups + 1, one_help, 0)

        def put(tile, carry):
            at = pl.ds(pl.multiple_of(tile * TILE, TILE), TILE)
            for i in range(blocks):
                part_out[tile, i] = total_h[at, i * LANE : (i + 1) * LANE].astype(jnp.bfloat16)
            part_copy(tile).start()
            return carry

        lax.fori_loop(0, tiles, put, 0)

    index_rows(index_a, near_a, ints_a)
    spread_index(index_a, matrix_a, spread, inv_a, weight)
    build_picks(spread, weight, sum_a, own_a, 0, half_chunks, near_base, 0, steps)

    @pl.when(inner)
    def _():
        lax.fori_loop(1, half, give_near, 0)
        build_picks(spread, weight, sum_a, own_a, half_chunks, half_chunks, far_base, 0, steps)

    spread_index(index_b, matrix_b, spread_b, inv_b, None)
    build_picks(spread_b, None, sum_b, own_b, 0, own_b.shape[0], 0, 0, seeds // (16 * PART))
    total[...] = jnp.zeros_like(total)
    live_groups = jnp.where(outer, half_groups, groups)

    def one_group(k, carry):
        @pl.when(k < live_groups)
        def _():
            take(group_of(k))

        @pl.when(k > 0)
        def _():
            group = group_of(k - 1)
            far = lax.div(turn_of(k - 1), half_groups)
            use(group, (lax.rem(group, half_groups) + far * half_groups) * deep)

        return carry

    lax.fori_loop(0, live_groups + 1, one_group, 0)

    def hide(tile, parts):
        at = pl.ds(pl.multiple_of(tile * TILE, TILE), TILE)
        inverse = inv_a[at, :]
        for b in range(2 * blocks):
            value = total[b // 2, at, (b % 2) * LANE : (b % 2 + 1) * LANE]
            if parts:
                value = value + part_in[b // blocks, tile, b % blocks].astype(jnp.float32)
            value = value * inverse + bias[0, :, b * LANE : (b + 1) * LANE]
            hidden[b, at, :] = jnp.maximum(value, 0.0).astype(jnp.bfloat16)

    @pl.when(inner)
    def _():
        def plain(tile, carry):
            hide(tile, False)
            return carry

        lax.fori_loop(0, tiles, plain, 0)

    @pl.when(outer)
    def _():
        def pass_on(tile, carry):
            part_copy(tile).wait_recv()
            part_relay(tile).start()
            return carry

        def joined(tile, carry):
            part_relay(tile).wait_recv()
            hide(tile, True)
            return carry

        lax.fori_loop(0, tiles, pass_on, 0)
        lax.fori_loop(0, tiles, joined, 0)

    hidden_all = across([hidden[b] for b in range(2 * blocks)])
    chunks_b = own_b.shape[0]
    own = dot(across([own_b[c] for c in range(chunks_b)]), hidden_all).astype(jnp.bfloat16)
    mean = dot(across([sum_b[c] for c in range(chunks_b)]), hidden_all)
    mean = (mean * across([inv_b[...]] * (2 * blocks))).astype(jnp.bfloat16)
    state = dot(own, across([wb[b, :hidden_width] for b in range(2 * blocks)]))
    state = state + dot(mean, across([wb[b, hidden_width:] for b in range(2 * blocks)]))
    state = jnp.maximum(state + bias[1], 0.0)
    squares = jnp.sum(state * state, axis=1, keepdims=True)
    scale = jnp.sqrt(jnp.float32(hidden_width)) / jnp.sqrt(squares + hidden_width)
    state = (state * scale).astype(out_ref.dtype)
    width = out_ref.shape[1]
    for c in range(2):
        @pl.when(core == c)
        def _():
            out_ref[...] = state[:, c * width : (c + 1) * width]

    others = pl.ds(0, n - 1)
    pltpu.make_async_copy(asked.at[others], wanted.at[others], ask_send).wait()

    @pl.when(outer)
    def _():
        for copy in index_copies:
            copy.wait_send()
        arrived(n - 2, send_sem)
        arrived(half, relay_send)
        arrived(half, help_relay_send)
        pltpu.make_async_copy(part_out, part_in.at[core], part_send).wait()
        pltpu.make_async_copy(part_in.at[core], part_in.at[partner], part_relay_send).wait()

    @pl.when(inner)
    def _():
        arrived(n - 1, send_sem)
        arrived(n, relay_send)


def shards(
    n,
    table,
    weight_a,
    bias_a,
    weight_b,
    bias_b,
    requests,
    near_a,
    self_a,
    count_a,
    near_b,
    self_b,
    count_b,
):
    each = requests.shape[2]
    half, half_hidden = table.shape[1], weight_a.shape[1]
    rows, seeds, slots = near_a.shape[0], near_b.shape[0], n * each
    wide = -(-(near_a.shape[1] + 2) // 8) * 8
    bf16, f32 = jnp.bfloat16, jnp.float32
    cols, blocks = half // LANE, half_hidden // LANE
    per = max(1, DEPTH // each)
    depth, groups = per * each, n // per
    args = (
        requests[0][:, None, :], table,
        near_a.T, self_a[None, :], count_a[None, :], near_b.T, self_b[None, :], count_b[None, :],
        weight_a, bias_a[None, :], weight_b, bias_b[None, :],
    )
    return pl.pallas_call(
        functools.partial(main_kernel, n),
        out_shape=pltpu.VMEM((seeds, half_hidden), bf16),
        in_specs=[ANY] * len(args),
        out_specs=VMEM,
        scratch_shapes=[
            pltpu.VMEM(args[0].shape, jnp.int32),
            pltpu.VMEM(table.shape, bf16),
            pltpu.VMEM(args[2].shape, jnp.int32),
            pltpu.VMEM((2, 1, rows), jnp.int32),
            pltpu.VMEM(args[5].shape, jnp.int32),
            pltpu.VMEM((2, 1, seeds), jnp.int32),
            pltpu.VMEM((2 * blocks, weight_a.shape[0], LANE), bf16),
            pltpu.VMEM((2 * blocks, weight_b.shape[0], LANE), bf16),
            pltpu.VMEM((2, 1, bias_a.shape[0]), f32),
            pltpu.VMEM((cols, table.shape[0], LANE), f32),
            pltpu.VMEM((n, 1, each), jnp.int32),
            pltpu.SMEM((n, 1, each), jnp.int32),
            pltpu.VMEM((cols, each, LANE), f32),
            pltpu.VMEM((n, cols, each, LANE), bf16),
            pltpu.VMEM((rows, wide), jnp.int32),
            pltpu.VMEM((seeds, wide), jnp.int32),
            pltpu.VMEM((2, n, cols, each, LANE), bf16),
            pltpu.VMEM((2, n // 2, cols, each, LANE), bf16),
            pltpu.VMEM(args[2].shape, jnp.int32),
            pltpu.VMEM((2, 1, rows), jnp.int32),
            pltpu.VMEM((2 * wide, (near_a.shape[1] + 2) * LANE), bf16),
            pltpu.VMEM((2 * wide, (near_b.shape[1] + 2) * LANE), bf16),
            pltpu.VMEM((near_a.shape[1] + 1, rows, LANE), jnp.int32),
            pltpu.VMEM((near_b.shape[1] + 1, seeds, LANE), jnp.int32),
            pltpu.VMEM((rows, LANE), f32),
            pltpu.VMEM((slots // LANE, rows, LANE), bf16),
            pltpu.VMEM((slots // LANE, rows, LANE), bf16),
            pltpu.VMEM((slots // LANE // 2, rows, LANE), bf16),
            pltpu.VMEM((slots // LANE // 2, rows, LANE), bf16),
            pltpu.VMEM((rows // LANE, seeds, LANE), bf16),
            pltpu.VMEM((rows // LANE, seeds, LANE), bf16),
            pltpu.VMEM((rows, LANE), f32),
            pltpu.VMEM((seeds, LANE), f32),
            pltpu.VMEM((2 * blocks, 2 * depth, LANE), bf16),
            pltpu.VMEM((blocks, rows, 2 * LANE), f32),
            pltpu.VMEM((blocks, 2 * depth, LANE), bf16),
            pltpu.VMEM((rows, half_hidden), f32),
            pltpu.VMEM((rows // TILE, blocks, TILE, LANE), bf16),
            pltpu.VMEM((2, rows // TILE, blocks, TILE, LANE), bf16),
            pltpu.VMEM((2 * blocks, rows, LANE), bf16),
            pltpu.SemaphoreType.DMA,
            pltpu.SemaphoreType.DMA((n,)),
            pltpu.SemaphoreType.DMA,
            pltpu.SemaphoreType.DMA((groups,)),
            pltpu.SemaphoreType.DMA,
            pltpu.SemaphoreType.DMA((groups,)),
            pltpu.SemaphoreType.DMA((2,)),
            pltpu.SemaphoreType.DMA((2,)),
            pltpu.SemaphoreType.DMA((9,)),
            pltpu.SemaphoreType.DMA((4,)),
            pltpu.SemaphoreType.DMA((2,)),
            pltpu.SemaphoreType.DMA((2,)),
            pltpu.SemaphoreType.DMA((groups // 2,)),
            pltpu.SemaphoreType.DMA,
            pltpu.SemaphoreType.DMA((groups // 2,)),
            pltpu.SemaphoreType.DMA,
            pltpu.SemaphoreType.DMA((rows // TILE,)),
            pltpu.SemaphoreType.DMA,
            pltpu.SemaphoreType.DMA((rows // TILE,)),
        ],
        compiler_params=pltpu.CompilerParams(
            collective_id=0, has_side_effects=True, vmem_limit_bytes=60 * 1024 * 1024
        ),
        name="sage",
    )(*args)


def solution(mesh):
    placed = (
        P("dom", "mp"),
        P(None, "mp"),
        P(),
        P(None, "mp"),
        P(),
        P("dom", None, None),
        P("dom", None),
        P("dom"),
        P("dom"),
        P("dom", None),
        P("dom"),
        P("dom"),
    )
    return jax.shard_map(
        functools.partial(shards, mesh.shape["dom"]),
        mesh=mesh, in_specs=placed, out_specs=P("dom", "mp"), check_vma=False,
    )
```
